128 devices in a mesh: seg: 64 (over x, z_hi, y, core), dir: 2 (over z_lo).
Axes of the slice: x: 4, y: 4, z: 4 (z_hi: 2, z_lo: 2; z = z_hi * 2 + z_lo), core: 2. Of those that a mesh axis runs over, the one named last changes fastest.
Arguments:
- strain: float32 [512, 8, 6, 8192], P('seg'), may hold values from -16 to 16
- valid_flags: int32 [512, 8], P('seg'), may hold values from 0 to 1, as said below
- direction_ids: int32 [1024], P('dir'), may hold values from 0 to 3071
- grid_patterns: float32 [3072, 6], replicated, may hold values from -1 to 1
- grid_delays: float32 [3072, 3], replicated, may hold values from -40 to 40
Outputs:
- peak: float32 [8, 8192], P(None, 'seg')
- dir_score: float32 [8, 1024], P(None, 'dir')
The draws below stay inside these ranges and needn't reach their ends.
Inputs may be any that keep to these rules, and one draw needn't show every extreme that they name: `valid_flags`: in every draw one window has no usable segment.
All inputs are finite; a program needn't handle non-finite values.
Results may differ from the reference program's by a relative error of at most 0.0001.
Values sent between devices are 32-bit elements; how exact they have to be, the bound alone decides.
A program may use at most 64 MiB of HBM per device.

```python
import math
import jax
import jax.numpy as jnp
from jax import lax

F = 8192
K = 1024
GRID = 3072
WIN = 8
SEGS = 512


def draw_valid_flags(key, part):
    key_levels, key_window = jax.random.split(jax.random.fold_in(key, 7331))
    levels = jax.random.randint(key_levels, (SEGS, WIN), 0, 4 * SEGS)
    position = jnp.arange(SEGS, dtype=jnp.int32)[:, None]
    usable = (levels < SEGS + 3 * position).astype(jnp.int32)
    silent_window = jax.random.randint(key_window, (), 0, WIN)
    keeper = (jnp.arange(WIN, dtype=jnp.int32)[None, :] != silent_window).astype(jnp.int32)
    return usable * keeper


def place_ends(array, rng, smallest, largest):
    spot = [jax.random.randint(jax.random.fold_in(rng, axis), (), 0, length) for axis, length in enumerate(array.shape)]
    longest = array.shape.index(max(array.shape))
    next_to = spot[:longest] + [(spot[longest] + 1) % array.shape[longest]] + spot[longest + 1:]
    return array.at[tuple(spot)].set(smallest).at[tuple(next_to)].set(largest)


def with_spikes(entries, stream_key, source, target, blocks, factor):
    owner, partner = [(jnp.arange(entries.shape[dim]) // (entries.shape[dim] // blocks)).reshape([-1 if axis == dim else 1 for axis in range(entries.ndim)]) for dim in (source, target)]
    chosen = jax.random.permutation(stream_key, blocks)[partner]
    strong = (owner == chosen) | (owner == (partner + blocks // 2) % blocks)
    return jnp.where(strong, factor * entries, entries)


def shard_levels(own_key, shape, pieces, smallest, top_value):
    def one(dim, blocks):
        draws = jax.random.uniform(jax.random.fold_in(jax.random.fold_in(own_key, 6), dim), (blocks,), jnp.float32, smallest / len(pieces), top_value / len(pieces))
        return jnp.repeat(jnp.exp(draws), shape[dim] // blocks).reshape((-1,) + (1,) * (len(shape) - dim - 1))

    loudness = one(*pieces[0])
    for cut in pieces[1:]:
        loudness = loudness * one(*cut)
    return loudness


def noise_with(own_key, shape, deviation, most, shards, heavy, held_as=jnp.bfloat16):
    entries = deviation * jax.random.normal(own_key, shape, jnp.float32)
    if shards:
        entries = entries * shard_levels(own_key, shape, shards, -0.22, 0.18)
    return jnp.clip(with_spikes(entries, jax.random.fold_in(own_key, 3), *heavy), -most, most).astype(held_as)


def setup_inputs(seed: int = 0) -> dict:
    seeds = jax.random.split(jax.random.key(seed), 6)
    strain = noise_with(seeds[0], (SEGS, WIN, 6, F), 1.0, 16.0, ((0, 64),), (0, 3, 64, 4.0), jnp.float32)
    valid_flags = draw_valid_flags(jax.random.fold_in(seeds[5], 71), 0)
    direction_ids = place_ends(jax.random.randint(seeds[2], (K,), 0, GRID), jax.random.fold_in(seeds[2], 1), 0, GRID - 1).astype(jnp.int32)
    grid_patterns = jnp.clip(jax.random.uniform(seeds[3], (GRID, 6), jnp.float32, -1.0, 1.0), -1.0, 1.0)
    grid_delays = jnp.clip(jax.random.uniform(seeds[4], (GRID, 3), jnp.float32, -40.0, 40.0), -40.0, 40.0)
    return dict(strain=strain, valid_flags=valid_flags, direction_ids=direction_ids, grid_patterns=grid_patterns, grid_delays=grid_delays)


PAIRS = ((0, 1), (0, 2), (1, 2))


def spectra(strain, valid_flags):
    weight = valid_flags.astype(jnp.float32)[:, :, None]
    real_part = strain[:, :, 0:3, :]
    imag_part = strain[:, :, 3:6, :]
    parts = []
    for d in range(3):
        parts.append(jnp.sum(weight * (real_part[:, :, d] * real_part[:, :, d] + imag_part[:, :, d] * imag_part[:, :, d]), 0))
    for d, e in PAIRS:
        parts.append(jnp.sum(weight * (real_part[:, :, d] * real_part[:, :, e] + imag_part[:, :, d] * imag_part[:, :, e]), 0))
    for d, e in PAIRS:
        parts.append(jnp.sum(weight * (imag_part[:, :, d] * real_part[:, :, e] - real_part[:, :, d] * imag_part[:, :, e]), 0))
    return jnp.stack(parts, 0)


def null_vectors(rows):
    plus = rows[:, 0:3]
    cross = rows[:, 3:6]
    first = plus[:, 1] * cross[:, 2] - plus[:, 2] * cross[:, 1]
    second = plus[:, 2] * cross[:, 0] - plus[:, 0] * cross[:, 2]
    third = plus[:, 0] * cross[:, 1] - plus[:, 1] * cross[:, 0]
    null = jnp.stack([first, second, third], 1)
    norm2 = jnp.maximum(jnp.sum(null * null, 1), 0.25)
    return null, norm2


def project(cov, first_bin, null, norm2, delays, count, total_bins):
    width = cov.shape[2]
    freq = (first_bin + jnp.arange(width, dtype=jnp.int32)).astype(jnp.float32) * (2.0 * math.pi / total_bins)
    energy = jnp.zeros((null.shape[0], cov.shape[1], width), jnp.float32)
    for d in range(3):
        energy = energy + (null[:, d] * null[:, d])[:, None, None] * cov[d][None]
    for index, (d, e) in enumerate(PAIRS):
        angle = (delays[:, d] - delays[:, e])[:, None] * freq[None, :]
        factor = (2.0 * null[:, d] * null[:, e])[:, None, None]
        energy = energy + factor * (jnp.cos(angle)[:, None, :] * cov[3 + index][None] + jnp.sin(angle)[:, None, :] * cov[6 + index][None])
    return energy / (norm2[:, None, None] * jnp.maximum(count, 1.0)[None, :, None])


def reference(strain, valid_flags, direction_ids, grid_patterns, grid_delays):
    cov = spectra(strain, valid_flags)
    count = jnp.sum(valid_flags.astype(jnp.float32), 0)
    rows = grid_patterns[direction_ids]
    delays = grid_delays[direction_ids]
    null, norm2 = null_vectors(rows)
    block = math.gcd(K, 64)
    blocks = K // block

    def one_block(items):
        power = project(cov, 0, items[0], items[1], items[2], count, F)
        return jnp.max(power, 0), jnp.sum(power, 2) / F

    peaks, scores = lax.map(one_block, (null.reshape(blocks, block, 3), norm2.reshape(blocks, block), delays.reshape(blocks, block, 3)))
    peak = jnp.max(peaks, 0)
    dir_score = scores.reshape(K, WIN).T
    return peak, dir_score
```

```python
import functools
import math

import jax
import jax.numpy as jnp
from jax import lax
from jax.experimental import pallas as pl
from jax.experimental.pallas import tpu as pltpu
from jax.sharding import PartitionSpec as P

F = 8192
PAIRS = ((0, 1), (0, 2), (1, 2))
FAR_FIRST = (2, 1, 3, 0)
MESH = pl.DeviceIdType.MESH
F32 = jnp.float32

SIN = [(-1.0) ** n * math.pi ** (2 * n + 1) / math.factorial(2 * n + 1) for n in range(7)]
COS = [(-1.0) ** n * math.pi ** (2 * n) / math.factorial(2 * n) for n in range(8)]


def horner(coefs, y):
    total = jnp.full_like(y, coefs[-1])
    for c in reversed(coefs[:-1]):
        total = total * y + c
    return total


def sincos_turns(u):
    r = u - jnp.round(u)
    y = r * r
    s = r * horner(SIN, y)
    c = horner(COS, y)
    return 2.0 * s * c, 1.0 - 2.0 * s * s


def kernel(
    strain, flags, ids, patterns, delays, peak_out, score_out,
    sb, part, cbuf, red, p1buf, s2buf, p2buf, plane, zbuf, cov,
    fl, idv, pat, dly, mask, lhs, coef, tab,
    acc, rbuf, pk, pkr,
    in_sem, st_sem, cs, cr, p1s, p1r, p2s, p2r, zs, zr, ds_, dr, es, er,
):
    me = lax.axis_index("seg")
    d = lax.axis_index("dir")
    core = lax.rem(me, 2)
    y = lax.rem(me // 2, 4)
    h = lax.rem(me // 8, 2)
    x = me // 16
    a = x + core * (y - x)
    b = y + core * (x - y)
    stride_a = 16 - 14 * core
    stride_b = 2 + 14 * core
    me_core = me + 1 - 2 * core
    me_h = me + 8 - 16 * h
    me_core_h = me_core + 8 - 16 * h

    def remote(src, dst, ssem, rsem, seg, dr_):
        return pltpu.make_async_remote_copy(
            src_ref=src, dst_ref=dst, send_sem=ssem, recv_sem=rsem,
            device_id=(seg, dr_), device_id_type=MESH)

    def along(j, at, stride):
        return me + (lax.rem(at + j, 4) - at) * stride

    barrier = pltpu.get_barrier_semaphore()
    friends = [(me_core, d), (me_h, d), (me, 1 - d), (me_h, 1 - d), (me_core_h, d)]
    for j in (1, 2, 3):
        friends += [(along(j, x, 16), d), (along(j, y, 2), d)]

    smalls = [
        pltpu.make_async_copy(flags, fl, in_sem.at[0]),
        pltpu.make_async_copy(ids, idv, in_sem.at[1]),
        pltpu.make_async_copy(patterns, pat, in_sem.at[2]),
        pltpu.make_async_copy(delays, dly, in_sem.at[3]),
    ]
    smalls[0].start()

    def chunk_copy(i, s):
        xp = lax.rem(x + FAR_FIRST[i], 4)
        start = pl.multiple_of((xp * 2 + d) * 1024, 1024)
        return pltpu.make_async_copy(
            strain.at[s, :, :, pl.ds(start, 1024)], sb.at[i, s], st_sem.at[i, s])

    for i in range(4):
        for s in range(8):
            chunk_copy(i, s).start()
    for c in smalls[1:]:
        c.start()
    for seg, dr_ in friends:
        pl.semaphore_signal(barrier, inc=1, device_id=(seg, dr_), device_id_type=MESH)

    smalls[0].wait()
    lane = lax.broadcasted_iota(jnp.int32, (8, 128), 1)
    sub8 = lax.broadcasted_iota(jnp.int32, (8, 8), 0)
    lane8 = lax.broadcasted_iota(jnp.int32, (8, 8), 1)
    fv = fl[...].astype(F32)
    count = jnp.zeros((8, 128), F32)
    for s in range(8):
        row = jnp.broadcast_to(fv[s : s + 1, :], (8, 8))
        col = jnp.sum(jnp.where(sub8 == lane8, row, 0.0), axis=1, keepdims=True)
        m = jnp.broadcast_to(col, (8, 128))
        mask[s] = m
        count = count + m

    def spectra(i, cc):
        def one(yp, carry):
            q = pl.multiple_of((yp * 2 + cc) * 128, 128)
            tot = [None] * 9

            def add(k, v):
                tot[k] = v if tot[k] is None else tot[k] + v

            for s in range(8):
                m = mask[s]
                re = [sb[i, s, e, :, pl.ds(q, 128)] * m for e in range(3)]
                im = [sb[i, s, e + 3, :, pl.ds(q, 128)] * m for e in range(3)]
                for e in range(3):
                    add(e, re[e] * re[e] + im[e] * im[e])
                for n, (e, g) in enumerate(PAIRS):
                    add(3 + n, re[e] * re[g] + im[e] * im[g])
                    add(6 + n, im[e] * re[g] - re[e] * im[g])
            for k in range(9):
                part[i, cc, yp, k] = tot[k]
            return carry

        lax.fori_loop(0, 4, one, 0)

    def core_copy(i):
        return remote(part.at[i, 1 - core], cbuf.at[i], cs.at[i], cr.at[i], me_core, d)

    def unit(i, j):
        xp = lax.rem(x + FAR_FIRST[i], 4)
        return xp + core * (j - xp), j + core * (xp - j)

    def p1_copy(i, j):
        ap, bp = unit(i, j)
        slot = lax.rem(ap - a + 4, 4) - 1
        return remote(red.at[ap, bp], p1buf.at[slot, bp], p1s.at[slot, bp],
                      p1r.at[slot, bp], me + (ap - a) * stride_a, d)

    def core_reduce(i):
        core_copy(i).wait_recv()
        for j in range(4):
            ap, bp = unit(i, j)
            red[ap, bp] = part[i, core, j] + cbuf[i, j]
        for j in range(4):
            ap, bp = unit(i, j)

            @pl.when(ap != a)
            def _():
                p1_copy(i, j).start()

    for i in range(4):
        for s in range(8):
            chunk_copy(i, s).wait()
        spectra(i, 1 - core)
        if i == 0:
            pl.semaphore_wait(barrier, len(friends))
        core_copy(i).start()
        spectra(i, core)
        if i > 0:
            core_reduce(i - 1)
    core_reduce(3)

    for c in smalls[1:]:
        c.wait()
    lhs[...] = jnp.zeros_like(lhs)
    for n, (src, rows) in enumerate(((pat, 6), (dly, 3))):
        v = src[...]
        hi = v.astype(jnp.bfloat16).astype(F32)
        rest = v - hi
        mid = rest.astype(jnp.bfloat16).astype(F32)
        lo = rest - mid
        lhs[8 * n : 8 * n + rows] = hi
        lhs[16 + 8 * n : 16 + 8 * n + rows] = mid
        lhs[32 + 8 * n : 32 + 8 * n + rows] = lo
    idrow = idv[...]

    def pick(g, got):
        base = pl.multiple_of(g * 256, 256)
        at = lax.broadcasted_iota(jnp.int32, (256, 512), 0) + base
        hot = jnp.where(at == idrow, 1.0, 0.0).astype(jnp.bfloat16)
        left = lhs[:, pl.ds(base, 256)].astype(jnp.bfloat16)
        return got + jnp.dot(left, hot, preferred_element_type=F32)

    got = lax.fori_loop(0, 12, pick, jnp.zeros((48, 512), F32))
    got = got[0:16] + got[16:32] + got[32:48]
    p = [got[n : n + 1] for n in range(6)]
    t = [got[8 + n : 9 + n] for n in range(3)]
    null = [
        p[1] * p[5] - p[2] * p[4],
        p[2] * p[3] - p[0] * p[5],
        p[0] * p[4] - p[1] * p[3],
    ]
    norm2 = jnp.maximum(null[0] * null[0] + null[1] * null[1] + null[2] * null[2], 0.25)
    inv = 1.0 / norm2
    rows = [n * n * inv for n in null]
    rows += [2.0 * null[e] * null[g] * inv for e, g in PAIRS]
    block = me.astype(F32) * (1.0 / 64.0)
    lags = [t[e] - t[g] for e, g in PAIRS]
    firsts = [v * block for v in lags]
    rows += [v - jnp.round(v) for v in firsts]
    rows += [v * (1.0 / F) for v in lags]
    rows += [jnp.zeros_like(inv)] * 4
    coef[...] = jnp.concatenate(rows, axis=0).T
    lanef = lane.astype(F32)

    def tables(g, carry):
        k = pl.multiple_of(g * 8, 8)
        c = coef[pl.ds(k, 8), :]

        def wide(n):
            return jnp.broadcast_to(c[:, n : n + 1], (8, 128))

        for n in range(3):
            tab[n, pl.ds(k, 8), :] = wide(n)
            sn, cn = sincos_turns(wide(6 + n) + wide(9 + n) * lanef)
            w = wide(3 + n)
            tab[3 + n, pl.ds(k, 8), :] = w * cn
            tab[6 + n, pl.ds(k, 8), :] = w * sn
        return carry

    lax.fori_loop(0, 64, tables, 0)

    def p1_wait(slot, bp):
        remote(red.at[a, bp], p1buf.at[slot, bp], p1s.at[slot, bp],
               p1r.at[slot, bp], me, d).wait_recv()

    def p2_copy(o):
        return remote(s2buf.at[o - 1], p2buf.at[o - 1], p2s.at[o - 1], p2r.at[o - 1],
                      along(o, b, stride_b), d)

    for o in (2, 1, 3):
        bp = lax.rem(b + o, 4)
        for slot in range(3):
            p1_wait(slot, bp)
        s2buf[o - 1] = (red[a, bp] + p1buf[0, bp]) + (p1buf[1, bp] + p1buf[2, bp])
        p2_copy(o).start()
    for slot in range(3):
        p1_wait(slot, b)
    own = (red[a, b] + p1buf[0, b]) + (p1buf[1, b] + p1buf[2, b])
    for o in (1, 2, 3):
        p2_copy(o).wait_recv()
    plane[...] = (own + p2buf[0]) + (p2buf[1] + p2buf[2])

    def z_copy(dd, n):
        return remote(plane, zbuf.at[h], zs.at[n], zr.at[h], me + (d - h) * 8, dd)

    @pl.when(h == d)
    def _():
        z_copy(1 - d, 0).start()

    @pl.when(h != d)
    def _():
        z_copy(0, 0).start()
        z_copy(1, 1).start()

    def z_wait(slot):
        remote(plane, zbuf.at[slot], zs.at[0], zr.at[slot], me, d).wait_recv()

    @pl.when(h == d)
    def _():
        z_wait(1 - h)
        cov[...] = plane[...] + zbuf[1 - h]

    @pl.when(h != d)
    def _():
        z_wait(0)
        z_wait(1)
        cov[...] = zbuf[0] + zbuf[1]

    cv = [cov[n] for n in range(9)]

    def outer(o, best):
        def inner(g, carry):
            best, score = carry
            for kk in range(8):
                k = o * 128 + g * 8 + kk
                e = None
                for n in range(9):
                    w = jnp.broadcast_to(tab[n, pl.ds(k, 1), :], (8, 128))
                    v = w * cv[n]
                    e = v if e is None else e + v
                best = jnp.maximum(best, e)
                s = jnp.sum(e, axis=1, keepdims=True)
                score = jnp.where(lane == g * 8 + kk, s, score)
            return best, score

        best, score = lax.fori_loop(0, 16, inner, (best, jnp.zeros((8, 128), F32)))
        acc[0, :, pl.ds(pl.multiple_of(o * 128, 128), 128)] = score
        return best

    best = lax.fori_loop(0, 4, outer, jnp.full((8, 128), -jnp.inf, F32))
    acc[0, :, 512:640] = count
    pk[...] = best

    pk_copy = remote(pk, pkr, es, er, me, 1 - d)
    pk_copy.start()

    groups = (
        ((me_core, 0), (me_h, 1), (me_core_h, 2)),
        tuple((along(o, a, stride_a), o - 1) for o in (2, 1, 3)),
        tuple((along(o, b, stride_b), o - 1) for o in (2, 1, 3)),
    )
    for n, group in enumerate(groups):
        copies = [
            remote(acc.at[n], rbuf.at[n, slot], ds_.at[n, slot], dr.at[n, slot], seg, d)
            for seg, slot in group
        ]
        for c in copies:
            c.start()
        for c in copies:
            c.wait_recv()
        acc[n + 1] = (acc[n] + rbuf[n, 0]) + (rbuf[n, 1] + rbuf[n, 2])

    inv_count = 1.0 / jnp.maximum(acc[3, :, 512:640], 1.0)
    for o in range(4):
        score_out[:, 128 * o : 128 * o + 128] = acc[3, :, 128 * o : 128 * o + 128] * inv_count * (1.0 / F)
    pk_copy.wait_recv()
    peak_out[...] = jnp.maximum(best, pkr[...]) * inv_count

    for i in range(4):
        core_copy(i).wait_send()
    for slot in range(3):
        for bp in range(4):
            remote(red.at[a, bp], p1buf.at[slot, bp], p1s.at[slot, bp],
                   p1r.at[slot, bp], me, d).wait_send()
    for o in (1, 2, 3):
        p2_copy(o).wait_send()
    z_copy(0, 0).wait_send()

    @pl.when(h != d)
    def _():
        z_copy(1, 1).wait_send()

    pk_copy.wait_send()
    for n, group in enumerate(groups):
        for seg, slot in group:
            remote(acc.at[n], rbuf.at[n, slot], ds_.at[n, slot], dr.at[n, slot], seg, d).wait_send()


def shards(strain, valid_flags, direction_ids, grid_patterns, grid_delays):
    unit = (9, 8, 128)
    dma = pltpu.SemaphoreType.DMA
    anywhere = pl.BlockSpec(memory_space=pl.ANY)
    vmem = pl.BlockSpec(memory_space=pltpu.VMEM)
    return pl.pallas_call(
        kernel,
        out_shape=(
            jax.ShapeDtypeStruct((8, 128), F32),
            jax.ShapeDtypeStruct((8, 512), F32),
        ),
        in_specs=[anywhere] * 5,
        out_specs=(vmem, vmem),
        scratch_shapes=[
            pltpu.VMEM((4, 8, 6, 8, 1024), F32),
            pltpu.VMEM((4, 2, 4) + unit, F32),
            pltpu.VMEM((4, 4) + unit, F32),
            pltpu.VMEM((4, 4) + unit, F32),
            pltpu.VMEM((3, 4) + unit, F32),
            pltpu.VMEM((3,) + unit, F32),
            pltpu.VMEM((3,) + unit, F32),
            pltpu.VMEM(unit, F32),
            pltpu.VMEM((2,) + unit, F32),
            pltpu.VMEM(unit, F32),
            pltpu.VMEM((8, 8), jnp.int32),
            pltpu.VMEM((1, 512), jnp.int32),
            pltpu.VMEM((6, 3072), F32),
            pltpu.VMEM((3, 3072), F32),
            pltpu.VMEM((8, 8, 128), F32),
            pltpu.VMEM((48, 3072), F32),
            pltpu.VMEM((512, 16), F32),
            pltpu.VMEM((9, 512, 128), F32),
            pltpu.VMEM((4, 8, 640), F32),
            pltpu.VMEM((3, 3, 8, 640), F32),
            pltpu.VMEM((8, 128), F32),
            pltpu.VMEM((8, 128), F32),
            dma((4,)), dma((4, 8)),
            dma((4,)), dma((4,)),
            dma((3, 4)), dma((3, 4)),
            dma((3,)), dma((3,)),
            dma((2,)), dma((2,)),
            dma((3, 3)), dma((3, 3)),
            dma(()), dma(()),
        ],
        compiler_params=pltpu.CompilerParams(collective_id=0, has_side_effects=True),
        name="sky",
    )(
        strain.transpose(0, 2, 1, 3),
        valid_flags,
        direction_ids.reshape(1, -1),
        grid_patterns.T,
        grid_delays.T,
    )


def solution(mesh):
    placed = (P("seg", None, None, None), P("seg", None), P("dir"), P(), P())
    return jax.shard_map(
        shards,
        mesh=mesh,
        in_specs=placed,
        out_specs=(P(None, "seg"), P(None, "dir")),
        check_vma=False,
    )
```
